256 devices in a mesh: rep: 2 (over z), stretch: 2 (over core), tp: 64 (over x, y).
Axes of the slice: x: 8, y: 8, z: 2, core: 2. Of those that a mesh axis runs over, the one named last changes fastest.
The devices are a block of a 8x8x16 slice.
Arguments:
- query: bfloat16 [4, 512, 3072], P(('rep', 'stretch'), 'tp'), parts along dimension 0, may hold values from -64 to 64
- stretch_kv: bfloat16 [2, 4, 512, 3072], P(None, ('rep', 'stretch'), 'tp'), parts along dimension 1, may hold values from -6 to 6
- history_kv: bfloat16 [2, 32768, 3072], P(None, ('rep', 'tp')), parts along dimension 1, may hold values from -6 to 6
- block_mask: int32 [4, 4, 8], P(('rep', 'stretch')), parts along dimension 0, may hold values from 0 to 1, as said below
- noise_level: int32 [4], P(('rep', 'stretch')), parts along dimension 0, may hold values from 0 to 999
- history_blocks: int32 [2], P('rep'), parts along dimension 0, may hold values from 1 to 128
- out_weight: bfloat16 [3072, 6144], P(None, 'tp'), may hold values from -0.109375 to 0.109375
- gate_table: float32 [1000, 6144], P(None, 'tp'), may hold values from -6 to 6
Outputs:
- mixed: bfloat16 [4, 512, 6144], P(('rep', 'stretch'), None, 'tp'), parts along dimension 0
The draws below stay inside these ranges and needn't reach their ends.
There are 2 independent parts, one for each index of `rep`. The reference program is written for one: setup_inputs(seed, part) draws one part's arguments, and reference() takes and returns one part's arrays. A program takes and returns all parts, laid end to end along the dimension named above; an argument that names none is the same for every part. Nothing has to cross between parts.
Inputs may be any that keep to these rules, and one draw needn't show every extreme that they name: block_mask[c, i, 4 + i] = 1 for every query block i; block_mask[0, i, j] = 0 for j < 4.
All inputs are finite; a program needn't handle non-finite values.
Results may differ from the reference program's by a relative error of at most 0.0049.
Values may be sent and summed in bfloat16 or wider, within the bound.
A program may use at most 128 MiB of HBM per device.

```python
import math
import jax
import jax.numpy as jnp
from jax import lax

D = 6144
H = 24
HD = 128
LEVELS = 1000
BLK = 128
CT = 512
QB = 4
HIST = 16384


def shared_draws(key):
    query_key = jax.random.fold_in(key, 101)
    history_key = jax.random.fold_in(key, 202)
    feature_width = H * HD
    history = jnp.clip(jax.random.normal(history_key, (2, HIST, feature_width), jnp.float32), -6.0, 6.0)
    queries = jnp.clip(2.0 * jax.random.normal(query_key, (2, CT, feature_width), jnp.float32), -12.0, 12.0)
    return (queries, history)


def draw_query(key, part):
    return shared_draws(key)[0].astype(jnp.bfloat16)


def draw_history_kv(key, part):
    return shared_draws(key)[1].astype(jnp.bfloat16)


def draw_block_mask(key, part):
    raw_bits = jax.random.randint(jax.random.fold_in(key, 404), (2, QB, 2 * QB), 0, 5)
    grid_rows = lax.broadcasted_iota(jnp.int32, (2, QB, 2 * QB), 1)
    grid_cols = lax.broadcasted_iota(jnp.int32, (2, QB, 2 * QB), 2)
    grid_stretches = lax.broadcasted_iota(jnp.int32, (2, QB, 2 * QB), 0)
    block_allow = jnp.where(raw_bits < 3, 1, 0)
    block_allow = jnp.where(grid_cols == grid_rows + QB, 1, block_allow)
    block_allow = jnp.where((grid_stretches == 0) & (grid_cols < QB), 0, block_allow)
    return block_allow.astype(jnp.int32)


def levels(rng, extent, shards, least, high):
    level = 1.0
    for position, parts in shards:
        heights = jax.random.uniform(jax.random.fold_in(jax.random.fold_in(rng, 6), position), (parts,), jnp.float32, least / len(shards), high / len(shards))
        level = level * jnp.repeat(jnp.exp(heights), extent[position] // parts).reshape((-1,) + (1,) * (len(extent) - 1 - position))
    return level


def bell_draw(own_key, dims, width, most, shards=(), kind=jnp.bfloat16):
    values = jax.random.normal(own_key, dims, jnp.float32) * width
    if len(shards) > 0:
        values = levels(own_key, dims, shards, -0.22, 0.18) * values
    return jnp.clip(values, min=-most, max=most).astype(kind)


def setup_inputs(seed: int = 0, part: int = 0) -> dict:
    key_list = jax.random.split(jax.random.key(seed), 9)
    own_keys = jax.random.split(jax.random.fold_in(key_list[8], part), 9)
    return {
        "query": draw_query(jax.random.fold_in(jax.random.fold_in(key_list[8], part), 71), part),
        "stretch_kv": bell_draw(own_keys[1], (2, 2, CT, H * HD), 1.0, 6.0, ((1, 2), (2, 64))),
        "history_kv": draw_history_kv(jax.random.fold_in(jax.random.fold_in(key_list[8], part), 71), part),
        "block_mask": draw_block_mask(jax.random.fold_in(jax.random.fold_in(key_list[8], part), 71), part),
        "noise_level": jax.random.randint(own_keys[4], (2,), 0, LEVELS).astype(jnp.int32),
        "history_blocks": jax.random.randint(own_keys[5], (1,), 1, HIST // BLK + 1).astype(jnp.int32),
        "out_weight": bell_draw(key_list[6], (H * HD, D), (H * HD) ** -0.5, 0.109375, ((1, 64),)),
        "gate_table": bell_draw(key_list[7], (LEVELS, D), 1.0, 6.0, ((1, 64),), jnp.float32),
    }


NEGATIVE = -1e+30

def single_head(triple_args, allowed):
    queries, key_rows, value_rows = triple_args
    scores = jnp.dot(queries, key_rows.T, preferred_element_type=jnp.float32) * (1.0 / math.sqrt(HD))
    scores = jnp.where(allowed, scores, NEGATIVE)
    row_peak = lax.optimization_barrier(jnp.max(scores, axis=1, keepdims=True))
    weights = jnp.where(allowed, jnp.exp(scores - row_peak), 0.0)
    weight_sum = lax.optimization_barrier(jnp.sum(weights, axis=1, keepdims=True))
    output = jnp.dot(weights, value_rows.astype(jnp.float32), precision=lax.Precision.HIGHEST) / weight_sum
    return output.astype(jnp.bfloat16)

def reference(query, stretch_kv, history_kv, block_mask, noise_level, history_blocks, out_weight, gate_table):
    history_live = jnp.arange(HIST, dtype=jnp.int32) < history_blocks[0] * BLK
    results = []
    for stretch_index in range(2):
        if stretch_index == 1:
            older_pair = stretch_kv[:, 0]
        else:
            older_pair = jnp.zeros_like(stretch_kv[:, 0])
        key_rows = jnp.concatenate([history_kv[0], older_pair[0], stretch_kv[0, stretch_index]], 0)
        value_rows = jnp.concatenate([history_kv[1], older_pair[1], stretch_kv[1, stretch_index]], 0)
        fresh = jnp.repeat(jnp.repeat(block_mask[stretch_index] > 0, BLK, axis=0), BLK, axis=1)
        allowed = jnp.concatenate([jnp.broadcast_to(history_live[None, :], (CT, HIST)), fresh], 1)
        key_count = key_rows.shape[0]
        head_queries = jnp.transpose(query[stretch_index].reshape(CT, H, HD), (1, 0, 2))
        head_keys = jnp.transpose(key_rows.reshape(key_count, H, HD), (1, 0, 2))
        head_values = jnp.transpose(value_rows.reshape(key_count, H, HD), (1, 0, 2))
        attended = lax.map(lambda triple_args: single_head(triple_args, allowed), (head_queries, head_keys, head_values))
        attended = jnp.transpose(attended, (1, 0, 2)).reshape(CT, H * HD)
        projected = jnp.dot(attended, out_weight, preferred_element_type=jnp.float32)
        gate_row = gate_table[noise_level[stretch_index]]
        results.append((projected * gate_row[None, :]).astype(jnp.bfloat16))
    return jnp.stack(results, 0)
```

```python
import functools
import math

import jax
import jax.numpy as jnp
from jax import lax
from jax.experimental import pallas as pl
from jax.experimental.pallas import tpu as pltpu
from jax.sharding import PartitionSpec as P

HD = 128
BLK = 128
NEGATIVE = -1e30
MESH = pl.DeviceIdType.MESH
F32 = jnp.float32
BF16 = jnp.bfloat16
EXP2_SCALE = math.log2(math.e) / math.sqrt(HD)


def remote(src, dst, send_sem, recv_sem, device):
    return pltpu.make_async_remote_copy(
        src_ref=src,
        dst_ref=dst,
        send_sem=send_sem,
        recv_sem=recv_sem,
        device_id=device,
        device_id_type=MESH,
    )


def dot(left, right, left_dim, right_dim):
    return lax.dot_general(
        left, right, (((left_dim,), (right_dim,)), ((), ())), preferred_element_type=F32
    )


def merged(parts):
    peak = parts[0][0]
    for part_peak, _, _ in parts[1:]:
        peak = jnp.maximum(peak, part_peak)
    total = None
    output = None
    for part_peak, part_sum, part_output in parts:
        weight = part_sum * jnp.exp2((part_peak - peak) * EXP2_SCALE)
        term = part_output.astype(F32) * weight
        total = weight if total is None else total + weight
        output = term if output is None else output + term
    return peak, total, output / total


def kernel(
    side,
    q_hbm,
    s_hbm,
    h_hbm,
    mask_sm,
    noise_sm,
    live_sm,
    w_hbm,
    g_hbm,
    out_ref,
    hist,
    qx,
    fx,
    msend,
    mtab,
    q1,
    q,
    kv,
    frb,
    obuf,
    stats,
    oa,
    oas,
    bbuf,
    ob,
    sb,
    fin,
    gath,
    wt,
    gate,
    loc,
    dds,
    ddr,
    q1s,
    q1r,
    q2s,
    q2r,
    kvs,
    kvr,
    frs,
    frr,
    oss,
    osr,
    sss,
    ssr,
    obs,
    obr,
    sbs,
    sbr,
    g1s,
    g1r,
    g2s,
    g2r,
):
    S = side
    half = S // 2
    R, F = q_hbm.shape
    HR = h_hbm.shape[1]
    T = S * S * R
    FG = F // 8
    HH = FG // HD
    FP = FG // half
    CB = T // half
    GR = math.gcd(FP, HD)
    QB = mask_sm.shape[1]
    NB = mask_sm.shape[2]

    e = lax.axis_index("stretch")
    t = lax.axis_index("tp")
    x = t // S
    y = t % S
    a = x + e * (y - x)
    b = y + e * (x - y)

    def tp_of(a_, b_):
        return (a_ + e * (b_ - a_)) * S + b_ + e * (a_ - b_)

    def at(a_, b_):
        return {"tp": tp_of(a_, b_)}

    other_core = {"stretch": 1 - e}

    def group_of(a_, b_):
        return (a_ % 2) * 4 + (b_ % 2) * 2 + e

    def partner(v):
        return (v + S + 1 - 2 * ((v + e) % 2)) % S

    a2 = partner(a)
    b2 = partner(b)
    block = [(a, b), (a2, b), (a, b2), (a2, b2)]
    ia = a // 2
    jb = b // 2

    ld_hist = pltpu.make_async_copy(h_hbm, hist, loc.at[0])
    ld_q = [
        pltpu.make_async_copy(
            q_hbm.at[:, pl.ds(p * (F // 2), F // 2)], qx.at[p, e], loc.at[1 + p]
        )
        for p in range(2)
    ]
    ld_f = pltpu.make_async_copy(s_hbm, fx.at[:, pl.ds(e * R, R), :], loc.at[3])
    ld_w = pltpu.make_async_copy(w_hbm, wt, loc.at[4])
    ld_g = pltpu.make_async_copy(g_hbm, gate, loc.at[5])
    for copy in ld_q + [ld_f, ld_hist, ld_w, ld_g]:
        copy.start()

    barrier = pltpu.get_barrier_semaphore()
    for k in range(1, S):
        for device in (at((a + k) % S, b), at(a, (b + k) % S)):
            pl.semaphore_signal(barrier, inc=1, device_id=device, device_id_type=MESH)
    for device in (at(a2, b2), other_core):
        pl.semaphore_signal(barrier, inc=1, device_id=device, device_id_type=MESH)

    lane = lax.broadcasted_iota(jnp.int32, (1, T), 1)
    swapped = ((lane // R) % S) * (S * R) + (lane // (S * R)) * R + lane % R
    own_order = jnp.where(e == 0, lane, swapped) // BLK
    other_order = jnp.where(e == 0, swapped, lane) // BLK
    for u in range(NB):
        own_row = jnp.zeros((1, T), F32)
        other_row = jnp.zeros((1, T), F32)
        for i in range(QB):
            bias = (mask_sm[0, i, u].astype(F32) - 1.0) * (-NEGATIVE)
            own_row = jnp.where(own_order == i, bias, own_row)
            other_row = jnp.where(other_order == i, bias, other_row)
        mtab[e, u] = own_row
        msend[u] = other_row

    for copy in ld_q + [ld_f]:
        copy.wait()
    pl.semaphore_wait(barrier, 2 * (S - 1) + 2)

    dq = remote(qx.at[:, e], qx.at[:, e], dds.at[0], ddr.at[0], other_core)
    df = remote(
        fx.at[:, pl.ds(e * R, R), :],
        fx.at[:, pl.ds(e * R, R), :],
        dds.at[1],
        ddr.at[1],
        other_core,
    )
    dm = remote(msend, mtab.at[e], dds.at[2], ddr.at[2], other_core)
    dq.start()
    df.start()
    dm.start()

    def q_cols(b_):
        return pl.ds(pl.multiple_of(((b_ % 2) * 2 + e) * FG, FG), FG)

    q1_rows = pl.ds(pl.multiple_of(b * R, R), R)

    def q1_copy(k):
        b_ = (b + k) % S
        return remote(
            qx.at[:, :, :, q_cols(b_)], q1.at[:, :, q1_rows, :], q1s.at[k], q1r.at[k], at(a, b_)
        )

    q1_own = pltpu.make_async_copy(qx.at[:, :, :, q_cols(b)], q1.at[:, :, q1_rows, :], loc.at[6])

    def kv_cols(p, h):
        start = group_of(*block[p]) * FG + h * HD
        return pl.ds(pl.multiple_of(start, HD), HD)

    def kv_copy(h, p):
        return remote(
            hist.at[:, :, kv_cols(p, h)], kv.at[h, p], kvs.at[h, p], kvr.at[h, p], at(*block[p])
        )

    def kv_own(h):
        return pltpu.make_async_copy(hist.at[:, :, kv_cols(0, h)], kv.at[h, 0], loc.at[8 + h])

    def f_cols(p):
        return pl.ds(pl.multiple_of(group_of(*block[p]) * FG, FG), FG)

    def f_copy(p):
        return remote(
            fx.at[:, :, f_cols(p)],
            frb.at[:, pl.ds(p * 2 * R, 2 * R), :],
            frs.at[p],
            frr.at[p],
            at(*block[p]),
        )

    f_own = pltpu.make_async_copy(
        fx.at[:, :, f_cols(0)], frb.at[:, pl.ds(0, 2 * R), :], loc.at[7]
    )

    q_rows = pl.ds(pl.multiple_of(a * (S * R), S * R), S * R)

    def h_cols(h):
        return pl.ds(pl.multiple_of(h * HD, HD), HD)

    def q2_copy(h, k):
        a_ = (a + k) % S
        return remote(
            q1.at[a_ % 2, :, :, h_cols(h)],
            q.at[h, :, q_rows, :],
            q2s.at[h, k],
            q2r.at[h, k],
            at(a_, b),
        )

    def q2_own(h):
        return pltpu.make_async_copy(
            q1.at[a % 2, :, :, h_cols(h)], q.at[h, :, q_rows, :], loc.at[8 + HH + h]
        )

    dq.wait_recv()
    for k in range(1, S):
        q1_copy(k).start()
    q1_own.start()
    ld_hist.wait()
    for p in (3, 1, 2):
        kv_copy(0, p).start()
    df.wait_recv()
    for p in (3, 1, 2):
        f_copy(p).start()
    for h in range(HH):
        kv_own(h).start()
    f_own.start()
    q1_own.wait()
    for k in range(1, S):
        q1_copy(k).wait_recv()
    for h in range(HH):
        if h > 0:
            for p in (3, 1, 2):
                kv_copy(h, p).start()
        for k in (4, 3, 5, 2, 6, 1, 7) if S == 8 else range(1, S):
            q2_copy(h, k).start()
        q2_own(h).start()

    dm.wait_recv()
    f_own.wait()
    for p in (1, 2, 3):
        f_copy(p).wait_recv()
    live = live_sm[0] * BLK

    def o_copy(h, k):
        i = (ia + k) % half
        return remote(
            obuf.at[h, k], oa.at[h, k], oss.at[h, k], osr.at[h, k], at(2 * i + a % 2, b)
        )

    def os_copy(h, k):
        i = (ia + k) % half
        return remote(
            stats.at[h, k], oas.at[h, k], sss.at[h, k], ssr.at[h, k], at(2 * i + a % 2, b)
        )

    def head(h, carry):
        kv_own(h).wait()
        q2_own(h).wait()
        for p in (1, 2, 3):
            kv_copy(h, p).wait_recv()
        for k in range(1, S):
            q2_copy(h, k).wait_recv()

        def chunk(n, carry):
            k = (n + 1) % half
            cols = pl.ds(pl.multiple_of(((ia + k) % half) * CB, CB), CB)
            queries = jnp.concatenate([q[h, 0, cols, :], q[h, 1, cols, :]], axis=0)
            scores = []
            for p in range(4):
                first = tp_of(*block[p]) * HR
                part = dot(kv[h, p, 0], queries, 1, 1)
                for r in range(HR // BLK):
                    bias = jnp.where(first + r * BLK < live, 0.0, NEGATIVE)
                    scores.append(part[r * BLK : (r + 1) * BLK] + bias)
            fresh_bias = []
            for p in range(4):
                u = (tp_of(*block[p]) * R) // BLK
                older = mtab[1, u, :, cols]
                own0 = mtab[0, QB + u, :, cols]
                own1 = mtab[1, QB + u, :, cols]
                none = jnp.full((1, CB), NEGATIVE, F32)
                for left, right in ((own0, older), (none, own1)):
                    row = jnp.concatenate([left, right], axis=1)
                    fresh_bias.append(jnp.broadcast_to(row, (R, 2 * CB)))
            fresh = dot(frb[0, :, h_cols(h)], queries, 1, 1) + jnp.concatenate(fresh_bias, axis=0)
            peak = jnp.max(fresh, axis=0, keepdims=True)
            for part in scores:
                peak = jnp.maximum(peak, jnp.max(part, axis=0, keepdims=True))
            weights = jnp.exp2((fresh - peak) * EXP2_SCALE)
            total = jnp.sum(weights, axis=0, keepdims=True)
            output = dot(frb[1, :, h_cols(h)], weights.astype(BF16), 0, 0)
            per = HR // BLK
            for p in range(4):
                block_weights = []
                for part in scores[p * per : (p + 1) * per]:
                    weights = jnp.exp2((part - peak) * EXP2_SCALE)
                    total = total + jnp.sum(weights, axis=0, keepdims=True)
                    block_weights.append(weights.astype(BF16))
                output = output + dot(
                    kv[h, p, 1], jnp.concatenate(block_weights, axis=0), 0, 0
                )
            output = (output / total).astype(BF16)
            obuf[h, k, 0] = output[:, :CB]
            obuf[h, k, 1] = output[:, CB:]
            stats[h, k] = jnp.concatenate(
                [peak[:, :CB], total[:, :CB], peak[:, CB:], total[:, CB:], jnp.zeros((4, CB), F32)],
                axis=0,
            )

            @pl.when(n >= 1)
            def _():
                o_copy(h, n).start()
                os_copy(h, n).start()

            return carry

        return lax.fori_loop(0, half, chunk, carry)

    lax.fori_loop(0, HH, head, 0)

    for h in range(HH):
        for k in range(1, half):
            o_copy(h, k).wait_recv()
            os_copy(h, k).wait_recv()
        for c in range(2):
            rows = slice(2 * c, 2 * c + 1)
            sums = slice(2 * c + 1, 2 * c + 2)
            parts = [(stats[h, 0, rows], stats[h, 0, sums], obuf[h, 0, c])]
            for k in range(1, half):
                parts.append((oas[h, k, rows], oas[h, k, sums], oa[h, k, c]))
            peak, total, output = merged(parts)
            bbuf[c, h * HD : (h + 1) * HD, :] = output.astype(BF16)
            row = (c * HH + h) * 2
            sb[0, row] = peak
            sb[0, row + 1] = total

    def b_copy(k):
        j = (jb + k) % half
        return remote(
            bbuf.at[:, pl.ds(pl.multiple_of(j * FP, GR), FP), :],
            ob.at[k],
            obs.at[k],
            obr.at[k],
            at(a, 2 * j + b % 2),
        )

    def bs_copy(k):
        j = (jb + k) % half
        return remote(sb.at[0], sb.at[k], sbs.at[k], sbr.at[k], at(a, 2 * j + b % 2))

    for k in range(1, half):
        bs_copy(k).start()
        b_copy(k).start()
    for k in range(1, half):
        bs_copy(k).wait_recv()
        b_copy(k).wait_recv()
    for c in range(2):
        for p in range(FP // GR):
            first = pl.multiple_of(jb * FP + p * GR, GR)
            row = (c * HH + first // HD) * 2
            parts = []
            for k in range(half):
                piece = (
                    bbuf[c, pl.ds(first, GR), :]
                    if k == 0
                    else ob[k, c, p * GR : (p + 1) * GR, :]
                )
                parts.append((sb[k, row], sb[k, row + 1], piece))
            _, _, output = merged(parts)
            fin[c, p * GR : (p + 1) * GR, :] = output.astype(BF16)

    gd = remote(fin.at[1 - e], gath.at[1, a, b], dds.at[3], ddr.at[3], other_core)
    gd.start()
    g_own = pltpu.make_async_copy(fin.at[e], gath.at[0, a, b], loc.at[8 + 2 * HH])
    g_own.start()

    def g1_copy(kind, k):
        dst = gath.at[0, a, b] if kind == 0 else gath.at[1, b, a]
        src = fin.at[e] if kind == 0 else gath.at[1, b, a]
        return remote(src, dst, g1s.at[kind, k], g1r.at[kind, k], at((a + k) % S, b))

    for k in range(1, S):
        g1_copy(0, k).start()
    gd.wait_recv()
    for k in range(1, S):
        g1_copy(1, k).start()
    g_own.wait()

    def g2_copy(d, s, kind):
        sign = 1 - 2 * d
        source = (b + S - sign * (s - 1)) % S
        slab = gath.at[0, :, source] if kind == 0 else gath.at[1, source]
        return remote(
            slab, slab, g2s.at[d, s, kind], g2r.at[d, s, kind], at(a, (b + S + sign) % S)
        )

    sent = []
    for s in range(1, half + 1):
        for kind in range(2):
            if s == 1:
                for k in range(1, S):
                    g1_copy(kind, k).wait_recv()
            for d in range(2):
                if s == half and kind != d:
                    continue
                if s > 1:
                    g2_copy(d, s - 1, kind).wait_recv()
                g2_copy(d, s, kind).start()
                sent.append((d, s, kind))
    for d in range(2):
        g2_copy(d, half - 1, 1 - d).wait_recv()
        g2_copy(d, half, d).wait_recv()

    ld_w.wait()
    ld_g.wait()
    results = []
    for kind in range(2):
        e_kind = e if kind == 0 else 1 - e
        result = None
        for pa in range(2):
            for pb in range(2):
                group = pa * 4 + pb * 2 + e_kind
                weight = wt[:, pl.ds(pl.multiple_of(group * FG, FG), FG)]
                rows = jnp.concatenate(
                    [
                        jnp.concatenate(
                            [gath[kind, 2 * i + pa, 2 * j + pb] for j in range(half)], axis=0
                        )
                        for i in range(half)
                    ],
                    axis=1,
                )
                term = dot(weight, rows, 1, 0)
                result = term if result is None else result + term
        results.append(result)
    natural = jnp.where(e == 0, results[0], results[1])
    crossed = jnp.where(e == 0, results[1], results[0])
    width = natural.shape[0]
    lanes = -(-width // 128) * 128
    if lanes > width:
        crossed = jnp.concatenate([crossed, jnp.zeros((lanes - width, T), F32)], axis=0)
    crossed = crossed.T
    crossed = jnp.concatenate(
        [
            crossed[(m * S + n) * R : (m * S + n + 1) * R]
            for n in range(S)
            for m in range(S)
        ],
        axis=0,
    )
    crossed = crossed.T[:width]
    levels = lax.broadcasted_iota(jnp.int32, gate.shape, 1)
    gate_column = jnp.sum(jnp.where(levels == noise_sm[0], gate[...], 0.0), axis=1, keepdims=True)
    out_ref[...] = ((natural + crossed) * gate_column).astype(BF16)

    for copy in (dq, df, dm, gd):
        copy.wait_send()
    for k in range(1, S):
        q1_copy(k).wait_send()
        g1_copy(0, k).wait_send()
        g1_copy(1, k).wait_send()
    for p in (1, 2, 3):
        f_copy(p).wait_send()
    for h in range(HH):
        for p in (1, 2, 3):
            kv_copy(h, p).wait_send()
        for k in range(1, S):
            q2_copy(h, k).wait_send()
        for k in range(1, half):
            o_copy(h, k).wait_send()
            os_copy(h, k).wait_send()
    for k in range(1, half):
        b_copy(k).wait_send()
        bs_copy(k).wait_send()
    for key in sent:
        g2_copy(*key).wait_send()


def on_device(
    side, query, stretch_kv, history_kv, block_mask, noise_level, history_blocks, out_weight, gate_table
):
    S = side
    half = S // 2
    R, F = query.shape[1:]
    HR = history_kv.shape[1]
    T = S * S * R
    FG = F // 8
    HH = FG // HD
    FP = FG // half
    CB = T // half
    C = out_weight.shape[1]
    DMA = pltpu.SemaphoreType.DMA
    any_space = pl.BlockSpec(memory_space=pl.ANY)
    smem = pl.BlockSpec(memory_space=pltpu.SMEM)
    out = pl.pallas_call(
        functools.partial(kernel, side),
        out_shape=jax.ShapeDtypeStruct((C, T), BF16),
        in_specs=[any_space, any_space, any_space, smem, smem, smem, any_space, any_space],
        out_specs=pl.BlockSpec(memory_space=pltpu.VMEM),
        scratch_shapes=[
            pltpu.VMEM((2, HR, F), BF16),
            pltpu.VMEM((2, 2, R, F // 2), BF16),
            pltpu.VMEM((2, 2 * R, F), BF16),
            pltpu.VMEM((block_mask.shape[2], 1, T), F32),
            pltpu.VMEM((2, block_mask.shape[2], 1, T), F32),
            pltpu.VMEM((2, 2, S * R, FG), BF16),
            pltpu.VMEM((HH, 2, T, HD), BF16),
            pltpu.VMEM((HH, 4, 2, HR, HD), BF16),
            pltpu.VMEM((2, 8 * R, FG), BF16),
            pltpu.VMEM((HH, half, 2, HD, CB), BF16),
            pltpu.VMEM((HH, half, 8, CB), F32),
            pltpu.VMEM((HH, half, 2, HD, CB), BF16),
            pltpu.VMEM((HH, half, 8, CB), F32),
            pltpu.VMEM((2, FG, CB), BF16),
            pltpu.VMEM((half, 2, FP, CB), BF16),
            pltpu.VMEM((half, 4 * HH, 1, CB), F32),
            pltpu.VMEM((2, FP, CB), BF16),
            pltpu.VMEM((2, S, S, FP, CB), BF16),
            pltpu.VMEM((C, F), BF16),
            pltpu.VMEM((C, gate_table.shape[0]), F32),
            DMA((9 + 2 * HH,)),
            DMA((4,)),
            DMA((4,)),
            DMA((S,)),
            DMA((S,)),
            DMA((HH, S)),
            DMA((HH, S)),
            DMA((HH, 4)),
            DMA((HH, 4)),
            DMA((4,)),
            DMA((4,)),
            DMA((HH, half)),
            DMA((HH, half)),
            DMA((HH, half)),
            DMA((HH, half)),
            DMA((half,)),
            DMA((half,)),
            DMA((half,)),
            DMA((half,)),
            DMA((2, S)),
            DMA((2, S)),
            DMA((2, half + 1, 2)),
            DMA((2, half + 1, 2)),
        ],
        compiler_params=pltpu.CompilerParams(
            collective_id=0, has_side_effects=True, vmem_limit_bytes=48 * 1024 * 1024
        ),
    )(
        query[0],
        stretch_kv[:, 0],
        history_kv,
        block_mask,
        noise_level,
        history_blocks,
        out_weight.T,
        gate_table.T,
    )
    return out.T[None]


def solution(mesh):
    side = math.isqrt(mesh.shape["tp"])
    return jax.shard_map(
        functools.partial(on_device, side),
        mesh=mesh,
        in_specs=(
            P(("rep", "stretch"), "tp", None),
            P(None, ("rep", "stretch"), "tp", None),
            P(None, ("rep", "tp"), None),
            P(("rep", "stretch"), None, None),
            P(("rep", "stretch")),
            P("rep"),
            P(None, "tp"),
            P(None, "tp"),
        ),
        out_specs=P(("rep", "stretch"), None, "tp"),
        check_vma=False,
    )
```

```python
import functools
import math

import jax
import jax.numpy as jnp
from jax import lax
from jax.experimental import pallas as pl
from jax.experimental.pallas import tpu as pltpu
from jax.sharding import PartitionSpec as P

HD = 128
BLK = 128
NEGATIVE = -1e30
MESH = pl.DeviceIdType.MESH
F32 = jnp.float32
BF16 = jnp.bfloat16
SMALL = 1e-30
STEP = 4
EXP2_SCALE = math.log2(math.e) / math.sqrt(HD)


def remote(src, dst, send_sem, recv_sem, device):
    return pltpu.make_async_remote_copy(
        src_ref=src,
        dst_ref=dst,
        send_sem=send_sem,
        recv_sem=recv_sem,
        device_id=device,
        device_id_type=MESH,
    )


def dot(left, right, left_dim, right_dim):
    return lax.dot_general(
        left, right, (((left_dim,), (right_dim,)), ((), ())), preferred_element_type=F32
    )


def merged(parts):
    peak = parts[0][0]
    for part_peak, _, _ in parts[1:]:
        peak = jnp.maximum(peak, part_peak)
    total = None
    output = None
    for part_peak, part_sum, part_output in parts:
        weight = part_sum * jnp.exp2((part_peak - peak) * EXP2_SCALE)
        term = part_output.astype(F32) * weight
        total = weight if total is None else total + weight
        output = term if output is None else output + term
    return peak, total, output / jnp.maximum(total, SMALL)


def kernel(
    side,
    q_hbm,
    s_hbm,
    h_hbm,
    mask_hbm,
    noise_hbm,
    live_hbm,
    w_hbm,
    g_hbm,
    out_ref,
    hist,
    qx,
    fx,
    msend,
    mtab,
    q1,
    q,
    kv,
    frb,
    obuf,
    stats,
    oa,
    oas,
    bbuf,
    ob,
    sb,
    fin,
    gath,
    wt,
    gate,
    mask_sm,
    noise_sm,
    live_sm,
    loc,
    dds,
    ddr,
    q1s,
    q1r,
    q2s,
    q2r,
    kvs,
    kvr,
    frs,
    frr,
    oss,
    osr,
    sss,
    ssr,
    obs,
    obr,
    sbs,
    sbr,
    g1s,
    g1r,
    g2s,
    g2r,
):
    S = side
    half = S // 2
    R, F = q_hbm.shape
    HR = h_hbm.shape[1]
    T = S * S * R
    FG = F // 8
    HH = FG // HD
    FP = FG // half
    CB = T // half
    GR = math.gcd(FP, HD)
    QB = mask_hbm.shape[1]
    NB = mask_hbm.shape[2]

    e = lax.axis_index("stretch")
    t = lax.axis_index("tp")
    x = t // S
    y = t % S
    a = x + e * (y - x)
    b = y + e * (x - y)

    def tp_of(a_, b_):
        return (a_ + e * (b_ - a_)) * S + b_ + e * (a_ - b_)

    def at(a_, b_):
        return {"tp": tp_of(a_, b_)}

    other_core = {"stretch": 1 - e}

    def group_of(a_, b_):
        return (a_ % 2) * 4 + (b_ % 2) * 2 + e

    def partner(v):
        return (v + S + 1 - 2 * ((v + e) % 2)) % S

    a2 = partner(a)
    b2 = partner(b)
    block = [(a, b), (a2, b), (a, b2), (a2, b2)]
    ia = a // 2
    jb = b // 2

    ld_hist = pltpu.make_async_copy(h_hbm, hist, loc.at[0])
    ld_q = [
        pltpu.make_async_copy(
            q_hbm.at[:, pl.ds(p * (F // 2), F // 2)], qx.at[p, e], loc.at[1 + p]
        )
        for p in range(2)
    ]
    ld_f = pltpu.make_async_copy(s_hbm, fx.at[:, pl.ds(e * R, R), :], loc.at[3])
    ld_w = pltpu.make_async_copy(w_hbm, wt, loc.at[4])
    ld_g = pltpu.make_async_copy(g_hbm, gate, loc.at[5])
    scalars = 9 + 2 * HH
    ld_mask = pltpu.make_async_copy(mask_hbm, mask_sm, loc.at[scalars])
    ld_noise = pltpu.make_async_copy(noise_hbm, noise_sm, loc.at[scalars + 1])
    ld_live = pltpu.make_async_copy(live_hbm, live_sm, loc.at[scalars + 2])
    for copy in ld_q + [ld_f, ld_mask, ld_noise, ld_live, ld_hist, ld_w, ld_g]:
        copy.start()

    barrier = pltpu.get_barrier_semaphore()
    for k in range(1, S):
        for device in (at((a + k) % S, b), at(a, (b + k) % S)):
            pl.semaphore_signal(barrier, inc=1, device_id=device, device_id_type=MESH)
    for device in (at(a2, b2), other_core):
        pl.semaphore_signal(barrier, inc=1, device_id=device, device_id_type=MESH)

    for copy in (ld_mask, ld_noise, ld_live):
        copy.wait()
    lane = lax.broadcasted_iota(jnp.int32, (1, T), 1)
    swapped = ((lane // R) % S) * (S * R) + (lane // (S * R)) * R + lane % R
    own_order = jnp.where(e == 0, lane, swapped) // BLK
    other_order = jnp.where(e == 0, swapped, lane) // BLK
    for u in range(NB):
        own_row = jnp.zeros((1, T), F32)
        other_row = jnp.zeros((1, T), F32)
        for i in range(QB):
            bias = (mask_sm[0, i, u].astype(F32) - 1.0) * (-NEGATIVE)
            own_row = jnp.where(own_order == i, bias, own_row)
            other_row = jnp.where(other_order == i, bias, other_row)
        mtab[e, u] = own_row
        msend[u] = other_row

    for copy in ld_q + [ld_f]:
        copy.wait()
    pl.semaphore_wait(barrier, 2 * (S - 1) + 2)

    dq = remote(qx.at[:, e], qx.at[:, e], dds.at[0], ddr.at[0], other_core)
    df = remote(
        fx.at[:, pl.ds(e * R, R), :],
        fx.at[:, pl.ds(e * R, R), :],
        dds.at[1],
        ddr.at[1],
        other_core,
    )
    dm = remote(msend, mtab.at[e], dds.at[2], ddr.at[2], other_core)
    dq.start()
    df.start()
    dm.start()

    def q_cols(b_):
        return pl.ds(pl.multiple_of(((b_ % 2) * 2 + e) * FG, FG), FG)

    q1_rows = pl.ds(pl.multiple_of(b * R, R), R)

    def q1_copy(k):
        b_ = (b + k) % S
        return remote(
            qx.at[:, :, :, q_cols(b_)], q1.at[:, :, q1_rows, :], q1s.at[k], q1r.at[k], at(a, b_)
        )

    q1_own = pltpu.make_async_copy(qx.at[:, :, :, q_cols(b)], q1.at[:, :, q1_rows, :], loc.at[6])

    def kv_cols(p, h):
        start = group_of(*block[p]) * FG + h * HD
        return pl.ds(pl.multiple_of(start, HD), HD)

    def kv_copy(h, p):
        return remote(
            hist.at[:, :, kv_cols(p, h)], kv.at[h, p], kvs.at[h, p], kvr.at[h, p], at(*block[p])
        )

    def kv_own(h):
        return pltpu.make_async_copy(hist.at[:, :, kv_cols(0, h)], kv.at[h, 0], loc.at[8 + h])

    def f_cols(p):
        return pl.ds(pl.multiple_of(group_of(*block[p]) * FG, FG), FG)

    def f_copy(p):
        return remote(
            fx.at[:, :, f_cols(p)],
            frb.at[:, pl.ds(p * 2 * R, 2 * R), :],
            frs.at[p],
            frr.at[p],
            at(*block[p]),
        )

    f_own = pltpu.make_async_copy(
        fx.at[:, :, f_cols(0)], frb.at[:, pl.ds(0, 2 * R), :], loc.at[7]
    )

    q_rows = pl.ds(pl.multiple_of(a * (S * R), S * R), S * R)

    def h_cols(h):
        return pl.ds(pl.multiple_of(h * HD, HD), HD)

    def q2_copy(h, k):
        a_ = (a + k) % S
        return remote(
            q1.at[a_ % 2, :, :, h_cols(h)],
            q.at[h, :, q_rows, :],
            q2s.at[h, k],
            q2r.at[h, k],
            at(a_, b),
        )

    def q2_own(h):
        return pltpu.make_async_copy(
            q1.at[a % 2, :, :, h_cols(h)], q.at[h, :, q_rows, :], loc.at[8 + HH + h]
        )

    dq.wait_recv()
    for k in range(1, S):
        q1_copy(k).start()
    q1_own.start()
    ld_hist.wait()
    for h in range(HH):
        for p in (3, 1, 2):
            kv_copy(h, p).start()
    df.wait_recv()
    for p in (3, 1, 2):
        f_copy(p).start()
    for h in range(HH):
        kv_own(h).start()
    f_own.start()
    q1_own.wait()
    for k in range(1, S):
        q1_copy(k).wait_recv()
    for h in range(HH):
        for k in (4, 3, 5, 2, 6, 1, 7) if S == 8 else range(1, S):
            q2_copy(h, k).start()
        q2_own(h).start()

    dm.wait_recv()
    f_own.wait()
    for p in (1, 2, 3):
        f_copy(p).wait_recv()
    live = live_sm[0] * BLK

    def o_copy(h, k):
        i = (ia + k) % half
        return remote(
            obuf.at[h, k], oa.at[h, k], oss.at[h, k], osr.at[h, k], at(2 * i + a % 2, b)
        )

    def os_copy(h, k):
        i = (ia + k) % half
        return remote(
            stats.at[h, k], oas.at[h, k], sss.at[h, k], ssr.at[h, k], at(2 * i + a % 2, b)
        )

    def head(h, carry):
        kv_own(h).wait()
        q2_own(h).wait()
        for p in (1, 2, 3):
            kv_copy(h, p).wait_recv()
        for k in range(1, S):
            q2_copy(h, k).wait_recv()

        def score(k):
            cols = pl.ds(pl.multiple_of(((ia + k) % half) * CB, CB), CB)
            queries = jnp.concatenate([q[h, 0, cols, :], q[h, 1, cols, :]], axis=0)
            fresh_bias = []
            for p in range(4):
                u = (tp_of(*block[p]) * R) // BLK
                older = mtab[1, u, :, cols]
                own0 = mtab[0, QB + u, :, cols]
                own1 = mtab[1, QB + u, :, cols]
                none = jnp.full((1, CB), NEGATIVE, F32)
                for left, right in ((own0, older), (none, own1)):
                    row = jnp.concatenate([left, right], axis=1)
                    fresh_bias.append(jnp.broadcast_to(row, (R, 2 * CB)))
            fresh = dot(frb[0, :, h_cols(h)], queries, 1, 1) + jnp.concatenate(fresh_bias, axis=0)
            scores = [fresh]
            for p in range(4):
                part = dot(kv[h, p, 0], queries, 1, 1)
                scores += [part[r * BLK : (r + 1) * BLK] for r in range(HR // BLK)]
            return scores

        per = HR // BLK
        alive = [
            tp_of(*block[p]) * HR + r * BLK < live for p in range(4) for r in range(per)
        ]

        def attend(k, scores):
            peak = jnp.max(scores[0], axis=0, keepdims=True)
            for part, on in zip(scores[1:], alive):
                top = jnp.max(part, axis=0, keepdims=True)
                peak = jnp.maximum(peak, jnp.where(on, top, NEGATIVE))
            weights = jnp.exp2(
                (scores[0] - jnp.where(peak > 0.5 * NEGATIVE, peak, -NEGATIVE)) * EXP2_SCALE
            )
            total = jnp.sum(weights, axis=0, keepdims=True)
            output = dot(frb[1, :, h_cols(h)], weights.astype(BF16), 0, 0)
            for p in range(4):
                block_weights = []
                for r in range(per):
                    shift = jnp.where(alive[p * per + r], peak, -NEGATIVE)
                    weights = jnp.exp2((scores[1 + p * per + r] - shift) * EXP2_SCALE)
                    total = total + jnp.sum(weights, axis=0, keepdims=True)
                    block_weights.append(weights.astype(BF16))
                output = output + dot(
                    kv[h, p, 1], jnp.concatenate(block_weights, axis=0), 0, 0
                )
            output = (output / jnp.maximum(total, SMALL)).astype(BF16)
            obuf[h, k, 0] = output[:, :CB]
            obuf[h, k, 1] = output[:, CB:]
            stats[h, k] = jnp.concatenate(
                [peak[:, :CB], total[:, :CB], peak[:, CB:], total[:, CB:], jnp.zeros((4, CB), F32)],
                axis=0,
            )

        def chunks(m, carry):
            ks = [(m * STEP + n + 1) % half for n in range(STEP)]
            all_scores = [score(k) for k in ks]
            for k, scores in zip(ks, all_scores):
                attend(k, scores)
            for k in ks:

                @pl.when(k > 0)
                def _():
                    o_copy(h, k).start()
                    os_copy(h, k).start()

            return carry

        return lax.fori_loop(0, half // STEP, chunks, carry)

    lax.fori_loop(0, HH, head, 0)

    for h in range(HH):
        for k in range(1, half):
            o_copy(h, k).wait_recv()
            os_copy(h, k).wait_recv()
        for c in range(2):
            rows = slice(2 * c, 2 * c + 1)
            sums = slice(2 * c + 1, 2 * c + 2)
            parts = [(stats[h, 0, rows], stats[h, 0, sums], obuf[h, 0, c])]
            for k in range(1, half):
                parts.append((oas[h, k, rows], oas[h, k, sums], oa[h, k, c]))
            peak, total, output = merged(parts)
            bbuf[c, h * HD : (h + 1) * HD, :] = output.astype(BF16)
            row = (c * HH + h) * 2
            sb[0, row] = peak
            sb[0, row + 1] = total

    def b_copy(k):
        j = (jb + k) % half
        return remote(
            bbuf.at[:, pl.ds(pl.multiple_of(j * FP, GR), FP), :],
            ob.at[k],
            obs.at[k],
            obr.at[k],
            at(a, 2 * j + b % 2),
        )

    def bs_copy(k):
        j = (jb + k) % half
        return remote(sb.at[0], sb.at[k], sbs.at[k], sbr.at[k], at(a, 2 * j + b % 2))

    for k in range(1, half):
        bs_copy(k).start()
        b_copy(k).start()
    for k in range(1, half):
        bs_copy(k).wait_recv()
        b_copy(k).wait_recv()
    for c in range(2):
        for p in range(FP // GR):
            first = pl.multiple_of(jb * FP + p * GR, GR)
            row = (c * HH + first // HD) * 2
            parts = []
            for k in range(half):
                piece = (
                    bbuf[c, pl.ds(first, GR), :]
                    if k == 0
                    else ob[k, c, p * GR : (p + 1) * GR, :]
                )
                parts.append((sb[k, row], sb[k, row + 1], piece))
            _, _, output = merged(parts)
            fin[c, p * GR : (p + 1) * GR, :] = output.astype(BF16)

    gd = remote(fin.at[1 - e], gath.at[b, a, 1], dds.at[3], ddr.at[3], other_core)
    gd.start()
    g_own = pltpu.make_async_copy(fin.at[e], gath.at[a, b, 0], loc.at[8 + 2 * HH])
    g_own.start()

    def g1_copy(kind, k):
        dst = gath.at[a, b, kind]
        src = fin.at[e] if kind == 0 else dst
        return remote(src, dst, g1s.at[kind, k], g1r.at[kind, k], at((a + k) % S, b))

    arrivals = [0] + [k for d in range(1, half) for k in (d, S - d)] + [half]
    for k in arrivals[1:]:
        g1_copy(0, k).start()
    gd.wait_recv()
    for k in arrivals[1:]:
        g1_copy(1, k).start()
    g_own.wait()

    def g2_copy(d, s, k):
        sign = 1 - 2 * d
        piece = gath.at[(a + S - k) % S, (b + S - sign * (s - 1)) % S]
        return remote(
            piece,
            piece,
            g2s.at[d, s - 1, k],
            g2r.at[d, s - 1, k],
            at(a, (b + S + sign) % S),
        )

    sends = [
        (place + S * (s - 1), s, d, k)
        for place, k in enumerate(arrivals)
        for s in range(1, half + 1)
        for d in range(2)
        if s < half or place % 2 == d
    ]
    sends = [key[1:] for key in sorted(sends)]
    for s, d, k in sends:
        if s == 1 and d == 0 and k > 0:
            g1_copy(0, k).wait_recv()
            g1_copy(1, k).wait_recv()
        if s > 1:
            g2_copy(d, s - 1, k).wait_recv()
        g2_copy(d, s, k).start()
    for s, d, k in sends:
        if (s + 1, d, k) not in sends:
            g2_copy(d, s, k).wait_recv()

    ld_w.wait()
    ld_g.wait()
    results = []
    for kind in range(2):
        e_kind = e if kind == 0 else 1 - e
        result = None
        for pa in range(2):
            for pb in range(2):
                group = pa * 4 + pb * 2 + e_kind
                weight = wt[:, pl.ds(pl.multiple_of(group * FG, FG), FG)]
                rows = jnp.concatenate(
                    [
                        jnp.concatenate(
                            [
                                gath[2 * i + pa, 2 * j + pb, 0]
                                if kind == 0
                                else gath[2 * j + pb, 2 * i + pa, 1]
                                for j in range(half)
                            ],
                            axis=0,
                        )
                        for i in range(half)
                    ],
                    axis=1,
                )
                term = dot(weight, rows, 1, 0)
                result = term if result is None else result + term
        results.append(result)
    natural = jnp.where(e == 0, results[0], results[1])
    crossed = jnp.where(e == 0, results[1], results[0])
    width = natural.shape[0]
    lanes = -(-width // 128) * 128
    if lanes > width:
        crossed = jnp.concatenate([crossed, jnp.zeros((lanes - width, T), F32)], axis=0)
    crossed = crossed.T
    crossed = jnp.concatenate(
        [
            crossed[(m * S + n) * R : (m * S + n + 1) * R]
            for n in range(S)
            for m in range(S)
        ],
        axis=0,
    )
    crossed = crossed.T[:width]
    levels = lax.broadcasted_iota(jnp.int32, gate.shape, 1)
    gate_column = jnp.sum(jnp.where(levels == noise_sm[0], gate[...], 0.0), axis=1, keepdims=True)
    out_ref[...] = ((natural + crossed) * gate_column).astype(BF16)

    for copy in (dq, df, dm):
        copy.wait_send()
    for k in range(1, S):
        q1_copy(k).wait_send()
    for p in (1, 2, 3):
        f_copy(p).wait_send()
    for h in range(HH):
        for p in (1, 2, 3):
            kv_copy(h, p).wait_send()
        for k in range(1, S):
            q2_copy(h, k).wait_send()
    for h in range(HH):
        for k in range(1, half):
            o_copy(h, k).wait_send()
            os_copy(h, k).wait_send()
    for k in range(1, half):
        b_copy(k).wait_send()
        bs_copy(k).wait_send()
    gd.wait_send()
    for k in range(1, S):
        g1_copy(0, k).wait_send()
        g1_copy(1, k).wait_send()
    for s, d, k in sends:
        g2_copy(d, s, k).wait_send()


def on_device(
    side, query, stretch_kv, history_kv, block_mask, noise_level, history_blocks, out_weight, gate_table
):
    S = side
    half = S // 2
    R, F = query.shape[1:]
    HR = history_kv.shape[1]
    T = S * S * R
    FG = F // 8
    HH = FG // HD
    FP = FG // half
    CB = T // half
    C = out_weight.shape[1]
    DMA = pltpu.SemaphoreType.DMA
    any_space = pl.BlockSpec(memory_space=pltpu.HBM)
    out = pl.pallas_call(
        functools.partial(kernel, side),
        out_shape=jax.ShapeDtypeStruct((C, T), BF16),
        in_specs=[any_space] * 8,
        out_specs=pl.BlockSpec(memory_space=pltpu.VMEM),
        scratch_shapes=[
            pltpu.VMEM((2, HR, F), BF16),
            pltpu.VMEM((2, 2, R, F // 2), BF16),
            pltpu.VMEM((2, 2 * R, F), BF16),
            pltpu.VMEM((block_mask.shape[2], 1, T), F32),
            pltpu.VMEM((2, block_mask.shape[2], 1, T), F32),
            pltpu.VMEM((2, 2, S * R, FG), BF16),
            pltpu.VMEM((HH, 2, T, HD), BF16),
            pltpu.VMEM((HH, 4, 2, HR, HD), BF16),
            pltpu.VMEM((2, 8 * R, FG), BF16),
            pltpu.VMEM((HH, half, 2, HD, CB), BF16),
            pltpu.VMEM((HH, half, 8, CB), F32),
            pltpu.VMEM((HH, half, 2, HD, CB), BF16),
            pltpu.VMEM((HH, half, 8, CB), F32),
            pltpu.VMEM((2, FG, CB), BF16),
            pltpu.VMEM((half, 2, FP, CB), BF16),
            pltpu.VMEM((half, 4 * HH, 1, CB), F32),
            pltpu.VMEM((2, FP, CB), BF16),
            pltpu.VMEM((S, S, 2, FP, CB), BF16),
            pltpu.VMEM((C, F), BF16),
            pltpu.VMEM((C, gate_table.shape[0]), F32),
            pltpu.SMEM(block_mask.shape, jnp.int32),
            pltpu.SMEM(noise_level.shape, jnp.int32),
            pltpu.SMEM(history_blocks.shape, jnp.int32),
            DMA((12 + 2 * HH,)),
            DMA((4,)),
            DMA((4,)),
            DMA((S,)),
            DMA((S,)),
            DMA((HH, S)),
            DMA((HH, S)),
            DMA((HH, 4)),
            DMA((HH, 4)),
            DMA((4,)),
            DMA((4,)),
            DMA((HH, half)),
            DMA((HH, half)),
            DMA((HH, half)),
            DMA((HH, half)),
            DMA((half,)),
            DMA((half,)),
            DMA((half,)),
            DMA((half,)),
            DMA((2, S)),
            DMA((2, S)),
            DMA((2, half, S)),
            DMA((2, half, S)),
        ],
        compiler_params=pltpu.CompilerParams(
            collective_id=0, has_side_effects=True, vmem_limit_bytes=63 * 1024 * 1024
        ),
    )(
        query[0],
        stretch_kv[:, 0],
        history_kv,
        block_mask,
        noise_level,
        history_blocks,
        out_weight.T,
        gate_table.T,
    )
    return out.T[None]


def solution(mesh):
    side = math.isqrt(mesh.shape["tp"])
    return jax.shard_map(
        functools.partial(on_device, side),
        mesh=mesh,
        in_specs=(
            P(("rep", "stretch"), "tp", None),
            P(None, ("rep", "stretch"), "tp", None),
            P(None, ("rep", "tp"), None),
            P(("rep", "stretch"), None, None),
            P(("rep", "stretch")),
            P("rep"),
            P(None, "tp"),
            P(None, "tp"),
        ),
        out_specs=P(("rep", "stretch"), None, "tp"),
        check_vma=False,
    )
```

```python
import functools
import math

import jax
import jax.numpy as jnp
from jax import lax
from jax.experimental import pallas as pl
from jax.experimental.pallas import tpu as pltpu
from jax.sharding import PartitionSpec as P

HD = 128
BLK = 128
NEGATIVE = -1e30
MESH = pl.DeviceIdType.MESH
F32 = jnp.float32
BF16 = jnp.bfloat16
SMALL = 1e-30
STEP = 4
EXP2_SCALE = math.log2(math.e) / math.sqrt(HD)


def remote(src, dst, send_sem, recv_sem, device):
    return pltpu.make_async_remote_copy(
        src_ref=src,
        dst_ref=dst,
        send_sem=send_sem,
        recv_sem=recv_sem,
        device_id=device,
        device_id_type=MESH,
    )


def dot(left, right, left_dim, right_dim):
    return lax.dot_general(
        left, right, (((left_dim,), (right_dim,)), ((), ())), preferred_element_type=F32
    )


def merged(parts):
    peak = parts[0][0]
    for part_peak, _, _ in parts[1:]:
        peak = jnp.maximum(peak, part_peak)
    total = None
    output = None
    for part_peak, part_sum, part_output in parts:
        weight = part_sum * jnp.exp2((part_peak - peak) * EXP2_SCALE)
        term = part_output.astype(F32) * weight
        total = weight if total is None else total + weight
        output = term if output is None else output + term
    return peak, total, output / jnp.maximum(total, SMALL)


def kernel(
    side,
    q_hbm,
    s_hbm,
    h_hbm,
    mask_hbm,
    noise_hbm,
    live_hbm,
    w_hbm,
    g_hbm,
    out_ref,
    hist,
    qx,
    fx,
    msend,
    mtab,
    q1,
    q,
    kv,
    frb,
    obuf,
    stats,
    oa,
    oas,
    bbuf,
    ob,
    sb,
    fin,
    gath,
    wt,
    gate,
    mask_sm,
    noise_sm,
    live_sm,
    loc,
    dds,
    ddr,
    q1s,
    q1r,
    q2s,
    q2r,
    kvs,
    kvr,
    frs,
    frr,
    oss,
    osr,
    sss,
    ssr,
    obs,
    obr,
    sbs,
    sbr,
    g1s,
    g1r,
    g2s,
    g2r,
):
    S = side
    half = S // 2
    R, F = q_hbm.shape
    HR = h_hbm.shape[1]
    T = S * S * R
    FG = F // 8
    HH = FG // HD
    FP = FG // half
    CB = T // half
    GR = math.gcd(FP, HD)
    QB = mask_hbm.shape[1]
    NB = mask_hbm.shape[2]

    e = lax.axis_index("stretch")
    t = lax.axis_index("tp")
    x = t // S
    y = t % S
    a = x + e * (y - x)
    b = y + e * (x - y)

    def tp_of(a_, b_):
        return (a_ + e * (b_ - a_)) * S + b_ + e * (a_ - b_)

    def at(a_, b_):
        return {"tp": tp_of(a_, b_)}

    def across(a_, b_):
        return {"stretch": 1 - e, "tp": tp_of(a_, b_)}

    other_core = {"stretch": 1 - e}

    def group_of(a_, b_):
        return (a_ % 2) * 4 + (b_ % 2) * 2 + e

    def partner(v):
        return (v + S + 1 - 2 * ((v + e) % 2)) % S

    a2 = partner(a)
    b2 = partner(b)
    block = [(a, b), (a2, b), (a, b2), (a2, b2)]
    ia = a // 2
    jb = b // 2

    ld_hist = pltpu.make_async_copy(h_hbm, hist, loc.at[0])
    ld_q = [
        pltpu.make_async_copy(
            q_hbm.at[:, pl.ds(p * (F // 2), F // 2)], qx.at[p], loc.at[1 + p]
        )
        for p in range(2)
    ]
    ld_f = pltpu.make_async_copy(s_hbm, fx.at[:, pl.ds(e * R, R), :], loc.at[3])
    ld_w = pltpu.make_async_copy(w_hbm, wt, loc.at[4])
    ld_g = pltpu.make_async_copy(g_hbm, gate, loc.at[5])
    scalars = 9 + 2 * HH
    ld_mask = pltpu.make_async_copy(mask_hbm, mask_sm, loc.at[scalars])
    ld_noise = pltpu.make_async_copy(noise_hbm, noise_sm, loc.at[scalars + 1])
    ld_live = pltpu.make_async_copy(live_hbm, live_sm, loc.at[scalars + 2])
    for copy in ld_q + [ld_f, ld_mask, ld_noise, ld_live, ld_hist, ld_w, ld_g]:
        copy.start()

    nearest = [0] + [k for d in range(1, half) for k in (d, S - d)] + [half]

    barrier = pltpu.get_barrier_semaphore()
    for k in range(1, S):
        for device in (
            at((a + k) % S, b),
            at(a, (b + k) % S),
            across((a + k) % S, b),
            across(a, (b + k) % S),
        ):
            pl.semaphore_signal(barrier, inc=1, device_id=device, device_id_type=MESH)
    for device in (at(a2, b2), other_core):
        pl.semaphore_signal(barrier, inc=1, device_id=device, device_id_type=MESH)

    for copy in (ld_mask, ld_noise, ld_live):
        copy.wait()
    lane = lax.broadcasted_iota(jnp.int32, (1, T), 1)
    swapped = ((lane // R) % S) * (S * R) + (lane // (S * R)) * R + lane % R
    own_order = jnp.where(e == 0, lane, swapped) // BLK
    other_order = jnp.where(e == 0, swapped, lane) // BLK
    for u in range(NB):
        own_row = jnp.zeros((1, T), F32)
        other_row = jnp.zeros((1, T), F32)
        for i in range(QB):
            bias = (mask_sm[0, i, u].astype(F32) - 1.0) * (-NEGATIVE)
            own_row = jnp.where(own_order == i, bias, own_row)
            other_row = jnp.where(other_order == i, bias, other_row)
        mtab[e, u] = own_row
        msend[u] = other_row

    for copy in ld_q + [ld_f]:
        copy.wait()
    pl.semaphore_wait(barrier, 4 * (S - 1) + 2)

    df = remote(
        fx.at[:, pl.ds(e * R, R), :],
        fx.at[:, pl.ds(e * R, R), :],
        dds.at[1],
        ddr.at[1],
        other_core,
    )
    dm = remote(msend, mtab.at[e], dds.at[2], ddr.at[2], other_core)
    df.start()
    dm.start()

    def q_cols(b_, core):
        return pl.ds(pl.multiple_of(((b_ % 2) * 2 + core) * FG, FG), FG)

    def q1_rows(b_):
        return pl.ds(pl.multiple_of(b_ * R, R), R)

    def q1_copy(k):
        b_ = (b + k) % S
        return remote(
            qx.at[:, :, q_cols(b_, e)],
            q1.at[:, e, q1_rows(b), :],
            q1s.at[0, k],
            q1r.at[0, k],
            at(a, b_),
        )

    def q1_across(k):
        a_ = (a + k) % S
        return remote(
            qx.at[:, :, q_cols(a_, 1 - e)],
            q1.at[:, e, q1_rows(a), :],
            q1s.at[1, k],
            q1r.at[1, k],
            across(a_, b),
        )

    q1_own = pltpu.make_async_copy(qx.at[:, :, q_cols(b, e)], q1.at[:, e, q1_rows(b), :], loc.at[6])

    def kv_cols(p, h):
        start = group_of(*block[p]) * FG + h * HD
        return pl.ds(pl.multiple_of(start, HD), HD)

    def kv_copy(h, p):
        return remote(
            hist.at[:, :, kv_cols(p, h)], kv.at[h, p], kvs.at[h, p], kvr.at[h, p], at(*block[p])
        )

    def kv_own(h):
        return pltpu.make_async_copy(hist.at[:, :, kv_cols(0, h)], kv.at[h, 0], loc.at[8 + h])

    def f_cols(p):
        return pl.ds(pl.multiple_of(group_of(*block[p]) * FG, FG), FG)

    def f_copy(p):
        return remote(
            fx.at[:, :, f_cols(p)],
            frb.at[:, pl.ds(p * 2 * R, 2 * R), :],
            frs.at[p],
            frr.at[p],
            at(*block[p]),
        )

    f_own = pltpu.make_async_copy(
        fx.at[:, :, f_cols(0)], frb.at[:, pl.ds(0, 2 * R), :], loc.at[7]
    )

    q_rows = pl.ds(pl.multiple_of(a * (S * R), S * R), S * R)

    def h_cols(h):
        return pl.ds(pl.multiple_of(h * HD, HD), HD)

    def q2_copy(h, k):
        a_ = (a + k) % S
        return remote(
            q1.at[a_ % 2, :, :, h_cols(h)],
            q.at[h, :, q_rows, :],
            q2s.at[h, k],
            q2r.at[h, k],
            at(a_, b),
        )

    def q2_own(h):
        return pltpu.make_async_copy(
            q1.at[a % 2, :, :, h_cols(h)], q.at[h, :, q_rows, :], loc.at[8 + HH + h]
        )

    for k in range(1, S):
        q1_copy(k).start()
        q1_across(k).start()
    q1_across(0).start()
    q1_own.start()
    ld_hist.wait()
    for p in (3, 1, 2):
        kv_copy(0, p).start()
    df.wait_recv()
    for p in (3, 1, 2):
        f_copy(p).start()
    for h in range(HH):
        kv_own(h).start()
    f_own.start()
    q1_own.wait()
    for k in range(S):
        q1_across(k).wait_recv()
        if k > 0:
            q1_copy(k).wait_recv()
    for h in range(HH):
        if h > 0:
            for p in (3, 1, 2):
                kv_copy(h, p).start()
        for k in reversed(nearest[1:]):
            q2_copy(h, k).start()
        q2_own(h).start()

    dm.wait_recv()
    f_own.wait()
    for p in (1, 2, 3):
        f_copy(p).wait_recv()
    live = live_sm[0] * BLK

    def o_copy(h, k):
        i = (ia + k) % half
        return remote(
            obuf.at[h, k], oa.at[h, k], oss.at[h, k], osr.at[h, k], at(2 * i + a % 2, b)
        )

    def os_copy(h, k):
        i = (ia + k) % half
        return remote(
            stats.at[h, k], oas.at[h, k], sss.at[h, k], ssr.at[h, k], at(2 * i + a % 2, b)
        )

    def head(h, carry):
        kv_own(h).wait()
        q2_own(h).wait()
        for p in (1, 2, 3):
            kv_copy(h, p).wait_recv()
        for k in range(1, S):
            q2_copy(h, k).wait_recv()

        def score(k):
            cols = pl.ds(pl.multiple_of(((ia + k) % half) * CB, CB), CB)
            queries = jnp.concatenate([q[h, 0, cols, :], q[h, 1, cols, :]], axis=0)
            fresh_bias = []
            for p in range(4):
                u = (tp_of(*block[p]) * R) // BLK
                older = mtab[1, u, :, cols]
                own0 = mtab[0, QB + u, :, cols]
                own1 = mtab[1, QB + u, :, cols]
                none = jnp.full((1, CB), NEGATIVE, F32)
                for left, right in ((own0, older), (none, own1)):
                    row = jnp.concatenate([left, right], axis=1)
                    fresh_bias.append(jnp.broadcast_to(row, (R, 2 * CB)))
            fresh = dot(frb[0, :, h_cols(h)], queries, 1, 1) + jnp.concatenate(fresh_bias, axis=0)
            scores = [fresh]
            for p in range(4):
                part = dot(kv[h, p, 0], queries, 1, 1)
                scores += [part[r * BLK : (r + 1) * BLK] for r in range(HR // BLK)]
            return scores

        per = HR // BLK
        alive = [
            tp_of(*block[p]) * HR + r * BLK < live for p in range(4) for r in range(per)
        ]

        def attend(k, scores):
            peak = jnp.max(scores[0], axis=0, keepdims=True)
            for part, on in zip(scores[1:], alive):
                top = jnp.max(part, axis=0, keepdims=True)
                peak = jnp.maximum(peak, jnp.where(on, top, NEGATIVE))
            weights = jnp.exp2(
                (scores[0] - jnp.where(peak > 0.5 * NEGATIVE, peak, -NEGATIVE)) * EXP2_SCALE
            )
            total = jnp.sum(weights, axis=0, keepdims=True)
            output = dot(frb[1, :, h_cols(h)], weights.astype(BF16), 0, 0)
            for p in range(4):
                block_weights = []
                for r in range(per):
                    shift = jnp.where(alive[p * per + r], peak, -NEGATIVE)
                    weights = jnp.exp2((scores[1 + p * per + r] - shift) * EXP2_SCALE)
                    total = total + jnp.sum(weights, axis=0, keepdims=True)
                    block_weights.append(weights.astype(BF16))
                output = output + dot(
                    kv[h, p, 1], jnp.concatenate(block_weights, axis=0), 0, 0
                )
            output = (output / jnp.maximum(total, SMALL)).astype(BF16)
            obuf[h, k, 0] = output[:, :CB]
            obuf[h, k, 1] = output[:, CB:]
            stats[h, k] = jnp.concatenate(
                [peak[:, :CB], total[:, :CB], peak[:, CB:], total[:, CB:], jnp.zeros((4, CB), F32)],
                axis=0,
            )

        def chunks(m, carry):
            ks = [(m * STEP + n + 1) % half for n in range(STEP)]
            all_scores = [score(k) for k in ks]
            for k, scores in zip(ks, all_scores):
                attend(k, scores)
            for k in ks:

                @pl.when(k > 0)
                def _():
                    o_copy(h, k).start()
                    os_copy(h, k).start()

            return carry

        return lax.fori_loop(0, half // STEP, chunks, carry)

    lax.fori_loop(0, HH, head, 0)

    for h in range(HH):
        for k in range(1, half):
            o_copy(h, k).wait_recv()
            os_copy(h, k).wait_recv()
        for c in range(2):
            rows = slice(2 * c, 2 * c + 1)
            sums = slice(2 * c + 1, 2 * c + 2)
            parts = [(stats[h, 0, rows], stats[h, 0, sums], obuf[h, 0, c])]
            for k in range(1, half):
                parts.append((oas[h, k, rows], oas[h, k, sums], oa[h, k, c]))
            peak, total, output = merged(parts)
            bbuf[c, h * HD : (h + 1) * HD, :] = output.astype(BF16)
            row = (c * HH + h) * 2
            sb[0, row] = peak
            sb[0, row + 1] = total

    def b_copy(k):
        j = (jb + k) % half
        return remote(
            bbuf.at[:, pl.ds(pl.multiple_of(j * FP, GR), FP), :],
            ob.at[k],
            obs.at[k],
            obr.at[k],
            at(a, 2 * j + b % 2),
        )

    def bs_copy(k):
        j = (jb + k) % half
        return remote(sb.at[0], sb.at[k], sbs.at[k], sbr.at[k], at(a, 2 * j + b % 2))

    for k in range(1, half):
        bs_copy(k).start()
        b_copy(k).start()
    for k in range(1, half):
        bs_copy(k).wait_recv()
        b_copy(k).wait_recv()
    for c in range(2):
        for p in range(FP // GR):
            first = pl.multiple_of(jb * FP + p * GR, GR)
            row = (c * HH + first // HD) * 2
            parts = []
            for k in range(half):
                piece = (
                    bbuf[c, pl.ds(first, GR), :]
                    if k == 0
                    else ob[k, c, p * GR : (p + 1) * GR, :]
                )
                parts.append((sb[k, row], sb[k, row + 1], piece))
            _, _, output = merged(parts)
            fin[c, p * GR : (p + 1) * GR, :] = output.astype(BF16)

    g_own = pltpu.make_async_copy(fin.at[e], gath.at[a, b, 0], loc.at[8 + 2 * HH])
    g_own.start()

    def g1_copy(k):
        return remote(
            fin.at[e], gath.at[a, b, 0], g1s.at[0, k], g1r.at[0, k], at((a + k) % S, b)
        )

    def g1_across(k):
        return remote(
            fin.at[1 - e], gath.at[b, a, 1], g1s.at[1, k], g1r.at[1, k], across(a, (b + k) % S)
        )

    arrivals = nearest
    for k in arrivals:
        g1_across(k).start()
        if k > 0:
            g1_copy(k).start()
    g_own.wait()
    g1_across(0).wait_recv()

    def g2_copy(d, s, k):
        sign = 1 - 2 * d
        piece = gath.at[(a + S - k) % S, (b + S - sign * (s - 1)) % S]
        return remote(
            piece,
            piece,
            g2s.at[d, s - 1, k],
            g2r.at[d, s - 1, k],
            at(a, (b + S + sign) % S),
        )

    sends = [
        (place + S * (s - 1), s, d, k)
        for place, k in enumerate(arrivals)
        for s in range(1, half + 1)
        for d in range(2)
        if s < half or place % 2 == d
    ]
    sends = [key[1:] for key in sorted(sends)]
    for s, d, k in sends:
        if s == 1 and d == 0 and k > 0:
            g1_copy(k).wait_recv()
            g1_across(k).wait_recv()
        if s > 1:
            g2_copy(d, s - 1, k).wait_recv()
        g2_copy(d, s, k).start()
    for s, d, k in sends:
        if (s + 1, d, k) not in sends:
            g2_copy(d, s, k).wait_recv()

    ld_w.wait()
    ld_g.wait()
    results = []
    for kind in range(2):
        e_kind = e if kind == 0 else 1 - e
        result = None
        for pa in range(2):
            for pb in range(2):
                group = pa * 4 + pb * 2 + e_kind
                weight = wt[:, pl.ds(pl.multiple_of(group * FG, FG), FG)]
                rows = jnp.concatenate(
                    [
                        jnp.concatenate(
                            [
                                gath[2 * i + pa, 2 * j + pb, 0]
                                if kind == 0
                                else gath[2 * j + pb, 2 * i + pa, 1]
                                for j in range(half)
                            ],
                            axis=0,
                        )
                        for i in range(half)
                    ],
                    axis=1,
                )
                term = dot(weight, rows, 1, 0)
                result = term if result is None else result + term
        results.append(result)
    natural = jnp.where(e == 0, results[0], results[1])
    crossed = jnp.where(e == 0, results[1], results[0])
    width = natural.shape[0]
    lanes = -(-width // 128) * 128
    if lanes > width:
        crossed = jnp.concatenate([crossed, jnp.zeros((lanes - width, T), F32)], axis=0)
    crossed = crossed.T
    crossed = jnp.concatenate(
        [
            crossed[(m * S + n) * R : (m * S + n + 1) * R]
            for n in range(S)
            for m in range(S)
        ],
        axis=0,
    )
    crossed = crossed.T[:width]
    levels = lax.broadcasted_iota(jnp.int32, gate.shape, 1)
    gate_column = jnp.sum(jnp.where(levels == noise_sm[0], gate[...], 0.0), axis=1, keepdims=True)
    out_ref[...] = ((natural + crossed) * gate_column).astype(BF16)

    for copy in (df, dm):
        copy.wait_send()
    for k in range(S):
        q1_across(k).wait_send()
        if k > 0:
            q1_copy(k).wait_send()
    for p in (1, 2, 3):
        f_copy(p).wait_send()
    for h in range(HH):
        for p in (1, 2, 3):
            kv_copy(h, p).wait_send()
        for k in range(1, S):
            q2_copy(h, k).wait_send()
    for h in range(HH):
        for k in range(1, half):
            o_copy(h, k).wait_send()
            os_copy(h, k).wait_send()
    for k in range(1, half):
        b_copy(k).wait_send()
        bs_copy(k).wait_send()
    for k in range(S):
        g1_across(k).wait_send()
        if k > 0:
            g1_copy(k).wait_send()
    for s, d, k in sends:
        g2_copy(d, s, k).wait_send()


def on_device(
    side, query, stretch_kv, history_kv, block_mask, noise_level, history_blocks, out_weight, gate_table
):
    S = side
    half = S // 2
    R, F = query.shape[1:]
    HR = history_kv.shape[1]
    T = S * S * R
    FG = F // 8
    HH = FG // HD
    FP = FG // half
    CB = T // half
    C = out_weight.shape[1]
    DMA = pltpu.SemaphoreType.DMA
    any_space = pl.BlockSpec(memory_space=pltpu.HBM)
    out = pl.pallas_call(
        functools.partial(kernel, side),
        out_shape=jax.ShapeDtypeStruct((C, T), BF16),
        in_specs=[any_space] * 8,
        out_specs=pl.BlockSpec(memory_space=pltpu.VMEM),
        scratch_shapes=[
            pltpu.VMEM((2, HR, F), BF16),
            pltpu.VMEM((2, R, F // 2), BF16),
            pltpu.VMEM((2, 2 * R, F), BF16),
            pltpu.VMEM((block_mask.shape[2], 1, T), F32),
            pltpu.VMEM((2, block_mask.shape[2], 1, T), F32),
            pltpu.VMEM((2, 2, S * R, FG), BF16),
            pltpu.VMEM((HH, 2, T, HD), BF16),
            pltpu.VMEM((HH, 4, 2, HR, HD), BF16),
            pltpu.VMEM((2, 8 * R, FG), BF16),
            pltpu.VMEM((HH, half, 2, HD, CB), BF16),
            pltpu.VMEM((HH, half, 8, CB), F32),
            pltpu.VMEM((HH, half, 2, HD, CB), BF16),
            pltpu.VMEM((HH, half, 8, CB), F32),
            pltpu.VMEM((2, FG, CB), BF16),
            pltpu.VMEM((half, 2, FP, CB), BF16),
            pltpu.VMEM((half, 4 * HH, 1, CB), F32),
            pltpu.VMEM((2, FP, CB), BF16),
            pltpu.VMEM((S, S, 2, FP, CB), BF16),
            pltpu.VMEM((C, F), BF16),
            pltpu.VMEM((C, gate_table.shape[0]), F32),
            pltpu.SMEM(block_mask.shape, jnp.int32),
            pltpu.SMEM(noise_level.shape, jnp.int32),
            pltpu.SMEM(history_blocks.shape, jnp.int32),
            DMA((12 + 2 * HH,)),
            DMA((4,)),
            DMA((4,)),
            DMA((2, S)),
            DMA((2, S)),
            DMA((HH, S)),
            DMA((HH, S)),
            DMA((HH, 4)),
            DMA((HH, 4)),
            DMA((4,)),
            DMA((4,)),
            DMA((HH, half)),
            DMA((HH, half)),
            DMA((HH, half)),
            DMA((HH, half)),
            DMA((half,)),
            DMA((half,)),
            DMA((half,)),
            DMA((half,)),
            DMA((2, S)),
            DMA((2, S)),
            DMA((2, half, S)),
            DMA((2, half, S)),
        ],
        compiler_params=pltpu.CompilerParams(
            collective_id=0, has_side_effects=True, vmem_limit_bytes=63 * 1024 * 1024
        ),
    )(
        query[0],
        stretch_kv[:, 0],
        history_kv,
        block_mask,
        noise_level,
        history_blocks,
        out_weight.T,
        gate_table.T,
    )
    return out.T[None]


def solution(mesh):
    side = math.isqrt(mesh.shape["tp"])
    return jax.shard_map(
        functools.partial(on_device, side),
        mesh=mesh,
        in_specs=(
            P(("rep", "stretch"), "tp", None),
            P(None, ("rep", "stretch"), "tp", None),
            P(None, ("rep", "tp"), None),
            P(("rep", "stretch"), None, None),
            P(("rep", "stretch")),
            P("rep"),
            P(None, "tp"),
            P(None, "tp"),
        ),
        out_specs=P(("rep", "stretch"), None, "tp"),
        check_vma=False,
    )
```

```python
import functools
import math

import jax
import jax.numpy as jnp
from jax import lax
from jax.experimental import pallas as pl
from jax.experimental.pallas import tpu as pltpu
from jax.sharding import PartitionSpec as P

HD = 128
BLK = 128
NEGATIVE = -1e30
MESH = pl.DeviceIdType.MESH
F32 = jnp.float32
BF16 = jnp.bfloat16
SMALL = 1e-30
STEP = 4
EXP2_SCALE = math.log2(math.e) / math.sqrt(HD)


def remote(src, dst, send_sem, recv_sem, device):
    return pltpu.make_async_remote_copy(
        src_ref=src,
        dst_ref=dst,
        send_sem=send_sem,
        recv_sem=recv_sem,
        device_id=device,
        device_id_type=MESH,
    )


def dot(left, right, left_dim, right_dim):
    return lax.dot_general(
        left, right, (((left_dim,), (right_dim,)), ((), ())), preferred_element_type=F32
    )


def merged(parts):
    peak = parts[0][0]
    for part_peak, _, _ in parts[1:]:
        peak = jnp.maximum(peak, part_peak)
    total = None
    output = None
    for part_peak, part_sum, part_output in parts:
        weight = part_sum * jnp.exp2((part_peak - peak) * EXP2_SCALE)
        term = part_output.astype(F32) * weight
        total = weight if total is None else total + weight
        output = term if output is None else output + term
    return peak, total, output / jnp.maximum(total, SMALL)


def kernel(
    side,
    q_hbm,
    s_hbm,
    h_hbm,
    mask_hbm,
    noise_hbm,
    live_hbm,
    w_hbm,
    g_hbm,
    out_ref,
    hist,
    qx,
    fx,
    msend,
    mtab,
    q1,
    q,
    kv,
    frb,
    obuf,
    stats,
    oa,
    oas,
    bbuf,
    ob,
    sb,
    fin,
    gath,
    wt,
    gate,
    mask_sm,
    noise_sm,
    live_sm,
    loc,
    dds,
    ddr,
    q1s,
    q1r,
    q2s,
    q2r,
    kvs,
    kvr,
    frs,
    frr,
    oss,
    osr,
    sss,
    ssr,
    obs,
    obr,
    sbs,
    sbr,
    g1s,
    g1r,
    g2s,
    g2r,
):
    S = side
    half = S // 2
    R, F = q_hbm.shape
    HR = h_hbm.shape[1]
    T = S * S * R
    FG = F // 8
    HH = FG // HD
    FP = FG // half
    CB = T // half
    GR = math.gcd(FP, HD)
    QB = mask_hbm.shape[1]
    NB = mask_hbm.shape[2]

    e = lax.axis_index("stretch")
    t = lax.axis_index("tp")
    x = t // S
    y = t % S
    a = x + e * (y - x)
    b = y + e * (x - y)

    def tp_of(a_, b_):
        return (a_ + e * (b_ - a_)) * S + b_ + e * (a_ - b_)

    def at(a_, b_):
        return {"tp": tp_of(a_, b_)}

    def across(a_, b_):
        return {"stretch": 1 - e, "tp": tp_of(a_, b_)}

    other_core = {"stretch": 1 - e}

    def group_of(a_, b_):
        return (a_ % 2) * 4 + (b_ % 2) * 2 + e

    def partner(v):
        return (v + S + 1 - 2 * ((v + e) % 2)) % S

    a2 = partner(a)
    b2 = partner(b)
    block = [(a, b), (a2, b), (a, b2), (a2, b2)]
    ia = a // 2
    jb = b // 2

    ld_hist = pltpu.make_async_copy(h_hbm, hist, loc.at[0])
    ld_q = [
        pltpu.make_async_copy(
            q_hbm.at[:, pl.ds(p * (F // 2), F // 2)], qx.at[p], loc.at[1 + p]
        )
        for p in range(2)
    ]
    ld_f = pltpu.make_async_copy(s_hbm, fx.at[:, pl.ds(e * R, R), :], loc.at[3])
    ld_w = pltpu.make_async_copy(w_hbm, wt, loc.at[4])
    ld_g = pltpu.make_async_copy(g_hbm, gate, loc.at[5])
    scalars = 9 + 2 * HH
    ld_mask = pltpu.make_async_copy(mask_hbm, mask_sm, loc.at[scalars])
    ld_noise = pltpu.make_async_copy(noise_hbm, noise_sm, loc.at[scalars + 1])
    ld_live = pltpu.make_async_copy(live_hbm, live_sm, loc.at[scalars + 2])
    for copy in ld_q + [ld_f, ld_mask, ld_noise, ld_live, ld_hist, ld_w, ld_g]:
        copy.start()

    nearest = [0] + [k for d in range(1, half) for k in (d, S - d)] + [half]

    barrier = pltpu.get_barrier_semaphore()
    for k in range(1, S):
        for device in (
            at((a + k) % S, b),
            at(a, (b + k) % S),
            across((a + k) % S, b),
            across(a, (b + k) % S),
        ):
            pl.semaphore_signal(barrier, inc=1, device_id=device, device_id_type=MESH)
    for device in (at(a2, b2), other_core):
        pl.semaphore_signal(barrier, inc=1, device_id=device, device_id_type=MESH)

    for copy in (ld_mask, ld_noise, ld_live):
        copy.wait()
    lane = lax.broadcasted_iota(jnp.int32, (1, T), 1)
    swapped = ((lane // R) % S) * (S * R) + (lane // (S * R)) * R + lane % R
    own_order = jnp.where(e == 0, lane, swapped) // BLK
    other_order = jnp.where(e == 0, swapped, lane) // BLK
    for u in range(NB):
        own_row = jnp.zeros((1, T), F32)
        other_row = jnp.zeros((1, T), F32)
        for i in range(QB):
            bias = (mask_sm[0, i, u].astype(F32) - 1.0) * (-NEGATIVE)
            own_row = jnp.where(own_order == i, bias, own_row)
            other_row = jnp.where(other_order == i, bias, other_row)
        mtab[e, u] = own_row
        msend[u] = other_row

    for copy in ld_q + [ld_f]:
        copy.wait()
    pl.semaphore_wait(barrier, 4 * (S - 1) + 2)

    df = remote(
        fx.at[:, pl.ds(e * R, R), :],
        fx.at[:, pl.ds(e * R, R), :],
        dds.at[1],
        ddr.at[1],
        other_core,
    )
    dm = remote(msend, mtab.at[e], dds.at[2], ddr.at[2], other_core)
    df.start()
    dm.start()

    def q_cols(b_, core):
        return pl.ds(pl.multiple_of(((b_ % 2) * 2 + core) * FG, FG), FG)

    def q1_rows(b_):
        return pl.ds(pl.multiple_of(b_ * R, R), R)

    def q1_copy(k):
        b_ = (b + k) % S
        return remote(
            qx.at[:, :, q_cols(b_, e)],
            q1.at[:, e, q1_rows(b), :],
            q1s.at[0, k],
            q1r.at[0, k],
            at(a, b_),
        )

    def q1_across(k):
        a_ = (a + k) % S
        return remote(
            qx.at[:, :, q_cols(a_, 1 - e)],
            q1.at[:, e, q1_rows(a), :],
            q1s.at[1, k],
            q1r.at[1, k],
            across(a_, b),
        )

    q1_own = pltpu.make_async_copy(qx.at[:, :, q_cols(b, e)], q1.at[:, e, q1_rows(b), :], loc.at[6])

    def kv_cols(p, h):
        start = group_of(*block[p]) * FG + h * HD
        return pl.ds(pl.multiple_of(start, HD), HD)

    def kv_copy(h, p):
        return remote(
            hist.at[:, :, kv_cols(p, h)], kv.at[h, p], kvs.at[h, p], kvr.at[h, p], at(*block[p])
        )

    def kv_own(h):
        return pltpu.make_async_copy(hist.at[:, :, kv_cols(0, h)], kv.at[h, 0], loc.at[8 + h])

    def f_cols(p):
        return pl.ds(pl.multiple_of(group_of(*block[p]) * FG, FG), FG)

    def f_copy(p):
        return remote(
            fx.at[:, :, f_cols(p)],
            frb.at[:, pl.ds(p * 2 * R, 2 * R), :],
            frs.at[p],
            frr.at[p],
            at(*block[p]),
        )

    f_own = pltpu.make_async_copy(
        fx.at[:, :, f_cols(0)], frb.at[:, pl.ds(0, 2 * R), :], loc.at[7]
    )

    q_rows = pl.ds(pl.multiple_of(a * (S * R), S * R), S * R)

    def h_cols(h):
        return pl.ds(pl.multiple_of(h * HD, HD), HD)

    def q2_copy(h, k):
        a_ = (a + k) % S
        return remote(
            q1.at[a_ % 2, :, :, h_cols(h)],
            q.at[h, :, q_rows, :],
            q2s.at[h, k],
            q2r.at[h, k],
            at(a_, b),
        )

    def q2_own(h):
        return pltpu.make_async_copy(
            q1.at[a % 2, :, :, h_cols(h)], q.at[h, :, q_rows, :], loc.at[8 + HH + h]
        )

    for k in reversed(nearest[1:]):
        q1_copy(k).start()
        q1_across(k).start()
    q1_across(0).start()
    q1_own.start()
    ld_hist.wait()
    for p in (3, 1, 2):
        kv_copy(0, p).start()
    df.wait_recv()
    for p in (3, 1, 2):
        f_copy(p).start()
    for h in range(HH):
        kv_own(h).start()
    f_own.start()
    q1_own.wait()
    for k in range(S):
        q1_across(k).wait_recv()
        if k > 0:
            q1_copy(k).wait_recv()
    for h in range(HH):
        if h > 0:
            for p in (3, 1, 2):
                kv_copy(h, p).start()
        for k in reversed(nearest[1:]):
            q2_copy(h, k).start()
        q2_own(h).start()

    dm.wait_recv()
    f_own.wait()
    for p in (1, 2, 3):
        f_copy(p).wait_recv()
    live = live_sm[0] * BLK

    def o_copy(h, k):
        i = (ia + k) % half
        return remote(
            obuf.at[h, k], oa.at[h, k], oss.at[h, k], osr.at[h, k], at(2 * i + a % 2, b)
        )

    def os_copy(h, k):
        i = (ia + k) % half
        return remote(
            stats.at[h, k], oas.at[h, k], sss.at[h, k], ssr.at[h, k], at(2 * i + a % 2, b)
        )

    def head(h, carry):
        kv_own(h).wait()
        q2_own(h).wait()
        for p in (1, 2, 3):
            kv_copy(h, p).wait_recv()
        for k in range(1, S):
            q2_copy(h, k).wait_recv()

        def score(k):
            cols = pl.ds(pl.multiple_of(((ia + k) % half) * CB, CB), CB)
            queries = jnp.concatenate([q[h, 0, cols, :], q[h, 1, cols, :]], axis=0)
            fresh_bias = []
            for p in range(4):
                u = (tp_of(*block[p]) * R) // BLK
                older = mtab[1, u, :, cols]
                own0 = mtab[0, QB + u, :, cols]
                own1 = mtab[1, QB + u, :, cols]
                none = jnp.full((1, CB), NEGATIVE, F32)
                for left, right in ((own0, older), (none, own1)):
                    row = jnp.concatenate([left, right], axis=1)
                    fresh_bias.append(jnp.broadcast_to(row, (R, 2 * CB)))
            fresh = dot(frb[0, :, h_cols(h)], queries, 1, 1) + jnp.concatenate(fresh_bias, axis=0)
            scores = [fresh]
            for p in range(4):
                part = dot(kv[h, p, 0], queries, 1, 1)
                scores += [part[r * BLK : (r + 1) * BLK] for r in range(HR // BLK)]
            return scores

        per = HR // BLK
        alive = [
            tp_of(*block[p]) * HR + r * BLK < live for p in range(4) for r in range(per)
        ]

        def attend(k, scores):
            peak = jnp.max(scores[0], axis=0, keepdims=True)
            for part, on in zip(scores[1:], alive):
                top = jnp.max(part, axis=0, keepdims=True)
                peak = jnp.maximum(peak, jnp.where(on, top, NEGATIVE))
            weights = jnp.exp2(
                (scores[0] - jnp.where(peak > 0.5 * NEGATIVE, peak, -NEGATIVE)) * EXP2_SCALE
            )
            total = jnp.sum(weights, axis=0, keepdims=True)
            output = dot(frb[1, :, h_cols(h)], weights.astype(BF16), 0, 0)
            for p in range(4):
                block_weights = []
                for r in range(per):
                    shift = jnp.where(alive[p * per + r], peak, -NEGATIVE)
                    weights = jnp.exp2((scores[1 + p * per + r] - shift) * EXP2_SCALE)
                    total = total + jnp.sum(weights, axis=0, keepdims=True)
                    block_weights.append(weights.astype(BF16))
                output = output + dot(
                    kv[h, p, 1], jnp.concatenate(block_weights, axis=0), 0, 0
                )
            output = (output / jnp.maximum(total, SMALL)).astype(BF16)
            obuf[h, k, 0] = output[:, :CB]
            obuf[h, k, 1] = output[:, CB:]
            stats[h, k] = jnp.concatenate(
                [peak[:, :CB], total[:, :CB], peak[:, CB:], total[:, CB:], jnp.zeros((4, CB), F32)],
                axis=0,
            )

        def chunks(m, carry):
            ks = [(m * STEP + n + 1) % half for n in range(STEP)]
            all_scores = [score(k) for k in ks]
            for k, scores in zip(ks, all_scores):
                attend(k, scores)
            for k in ks:

                @pl.when(k > 0)
                def _():
                    o_copy(h, k).start()
                    os_copy(h, k).start()

            return carry

        return lax.fori_loop(0, half // STEP, chunks, carry)

    lax.fori_loop(0, HH, head, 0)

    for h in range(HH):
        for k in range(1, half):
            o_copy(h, k).wait_recv()
            os_copy(h, k).wait_recv()
        for c in range(2):
            rows = slice(2 * c, 2 * c + 1)
            sums = slice(2 * c + 1, 2 * c + 2)
            parts = [(stats[h, 0, rows], stats[h, 0, sums], obuf[h, 0, c])]
            for k in range(1, half):
                parts.append((oas[h, k, rows], oas[h, k, sums], oa[h, k, c]))
            peak, total, output = merged(parts)
            bbuf[c, h * HD : (h + 1) * HD, :] = output.astype(BF16)
            row = (c * HH + h) * 2
            sb[0, row] = peak
            sb[0, row + 1] = total

    def b_copy(k):
        j = (jb + k) % half
        return remote(
            bbuf.at[:, pl.ds(pl.multiple_of(j * FP, GR), FP), :],
            ob.at[k],
            obs.at[k],
            obr.at[k],
            at(a, 2 * j + b % 2),
        )

    def bs_copy(k):
        j = (jb + k) % half
        return remote(sb.at[0], sb.at[k], sbs.at[k], sbr.at[k], at(a, 2 * j + b % 2))

    for k in range(1, half):
        bs_copy(k).start()
        b_copy(k).start()
    for copy in (df, dm):
        copy.wait_send()
    for k in range(S):
        q1_across(k).wait_send()
        if k > 0:
            q1_copy(k).wait_send()
    for p in (1, 2, 3):
        f_copy(p).wait_send()
    for h in range(HH):
        for p in (1, 2, 3):
            kv_copy(h, p).wait_send()
        for k in range(1, S):
            q2_copy(h, k).wait_send()
    for h in range(HH):
        for k in range(1, half):
            o_copy(h, k).wait_send()
            os_copy(h, k).wait_send()
    ld_g.wait()
    levels = lax.broadcasted_iota(jnp.int32, gate.shape, 1)
    gate_column = jnp.sum(jnp.where(levels == noise_sm[0], gate[...], 0.0), axis=1, keepdims=True)
    for k in range(1, half):
        bs_copy(k).wait_recv()
        b_copy(k).wait_recv()
    for c in range(2):
        for p in range(FP // GR):
            first = pl.multiple_of(jb * FP + p * GR, GR)
            row = (c * HH + first // HD) * 2
            parts = []
            for k in range(half):
                piece = (
                    bbuf[c, pl.ds(first, GR), :]
                    if k == 0
                    else ob[k, c, p * GR : (p + 1) * GR, :]
                )
                parts.append((sb[k, row], sb[k, row + 1], piece))
            _, _, output = merged(parts)
            fin[c, p * GR : (p + 1) * GR, :] = output.astype(BF16)

    g_own = pltpu.make_async_copy(fin.at[e], gath.at[a, b, 0], loc.at[8 + 2 * HH])
    g_own.start()

    def g1_copy(k):
        return remote(
            fin.at[e], gath.at[a, b, 0], g1s.at[0, k], g1r.at[0, k], at((a + k) % S, b)
        )

    def g1_across(k):
        return remote(
            fin.at[1 - e], gath.at[b, a, 1], g1s.at[1, k], g1r.at[1, k], across(a, (b + k) % S)
        )

    arrivals = nearest
    for k in arrivals:
        g1_across(k).start()
        if k > 0:
            g1_copy(k).start()
    g_own.wait()
    g1_across(0).wait_recv()

    def g2_copy(d, s, k):
        sign = 1 - 2 * d
        piece = gath.at[(a + S - k) % S, (b + S - sign * (s - 1)) % S]
        return remote(
            piece,
            piece,
            g2s.at[d, s - 1, k],
            g2r.at[d, s - 1, k],
            at(a, (b + S + sign) % S),
        )

    sends = [
        (place + S * (s - 1), s, d, k)
        for place, k in enumerate(arrivals)
        for s in range(1, half + 1)
        for d in range(2)
        if s < half or place % 2 == d
    ]
    sends = [key[1:] for key in sorted(sends)]
    for s, d, k in sends:
        if s == 1 and d == 0 and k > 0:
            g1_copy(k).wait_recv()
            g1_across(k).wait_recv()
        if s > 1:
            g2_copy(d, s - 1, k).wait_recv()
        g2_copy(d, s, k).start()
    for k in range(1, half):
        b_copy(k).wait_send()
        bs_copy(k).wait_send()
    for k in range(S):
        g1_across(k).wait_send()
        if k > 0:
            g1_copy(k).wait_send()
    for s, d, k in sends:
        g2_copy(d, s, k).wait_send()
    for s, d, k in sends:
        if (s + 1, d, k) not in sends:
            g2_copy(d, s, k).wait_recv()

    ld_w.wait()
    results = []
    for kind in range(2):
        e_kind = e if kind == 0 else 1 - e
        result = None
        for pa in range(2):
            for pb in range(2):
                group = pa * 4 + pb * 2 + e_kind
                weight = wt[:, pl.ds(pl.multiple_of(group * FG, FG), FG)]
                rows = jnp.concatenate(
                    [
                        jnp.concatenate(
                            [
                                gath[2 * i + pa, 2 * j + pb, 0]
                                if kind == 0
                                else gath[2 * j + pb, 2 * i + pa, 1]
                                for j in range(half)
                            ],
                            axis=0,
                        )
                        for i in range(half)
                    ],
                    axis=1,
                )
                term = dot(weight, rows, 1, 0)
                result = term if result is None else result + term
        results.append(result)
    natural = jnp.where(e == 0, results[0], results[1])
    crossed = jnp.where(e == 0, results[1], results[0])
    width = natural.shape[0]
    lanes = -(-width // 128) * 128
    if lanes > width:
        crossed = jnp.concatenate([crossed, jnp.zeros((lanes - width, T), F32)], axis=0)
    crossed = crossed.T
    crossed = jnp.concatenate(
        [
            crossed[(m * S + n) * R : (m * S + n + 1) * R]
            for n in range(S)
            for m in range(S)
        ],
        axis=0,
    )
    crossed = crossed.T[:width]
    out_ref[...] = ((natural + crossed) * gate_column).astype(BF16)


def on_device(
    side, query, stretch_kv, history_kv, block_mask, noise_level, history_blocks, out_weight, gate_table
):
    S = side
    half = S // 2
    R, F = query.shape[1:]
    HR = history_kv.shape[1]
    T = S * S * R
    FG = F // 8
    HH = FG // HD
    FP = FG // half
    CB = T // half
    C = out_weight.shape[1]
    DMA = pltpu.SemaphoreType.DMA
    any_space = pl.BlockSpec(memory_space=pltpu.HBM)
    out = pl.pallas_call(
        functools.partial(kernel, side),
        out_shape=jax.ShapeDtypeStruct((C, T), BF16),
        in_specs=[any_space] * 8,
        out_specs=pl.BlockSpec(memory_space=pltpu.VMEM),
        scratch_shapes=[
            pltpu.VMEM((2, HR, F), BF16),
            pltpu.VMEM((2, R, F // 2), BF16),
            pltpu.VMEM((2, 2 * R, F), BF16),
            pltpu.VMEM((block_mask.shape[2], 1, T), F32),
            pltpu.VMEM((2, block_mask.shape[2], 1, T), F32),
            pltpu.VMEM((2, 2, S * R, FG), BF16),
            pltpu.VMEM((HH, 2, T, HD), BF16),
            pltpu.VMEM((HH, 4, 2, HR, HD), BF16),
            pltpu.VMEM((2, 8 * R, FG), BF16),
            pltpu.VMEM((HH, half, 2, HD, CB), BF16),
            pltpu.VMEM((HH, half, 8, CB), F32),
            pltpu.VMEM((HH, half, 2, HD, CB), BF16),
            pltpu.VMEM((HH, half, 8, CB), F32),
            pltpu.VMEM((2, FG, CB), BF16),
            pltpu.VMEM((half, 2, FP, CB), BF16),
            pltpu.VMEM((half, 4 * HH, 1, CB), F32),
            pltpu.VMEM((2, FP, CB), BF16),
            pltpu.VMEM((S, S, 2, FP, CB), BF16),
            pltpu.VMEM((C, F), BF16),
            pltpu.VMEM((C, gate_table.shape[0]), F32),
            pltpu.SMEM(block_mask.shape, jnp.int32),
            pltpu.SMEM(noise_level.shape, jnp.int32),
            pltpu.SMEM(history_blocks.shape, jnp.int32),
            DMA((12 + 2 * HH,)),
            DMA((4,)),
            DMA((4,)),
            DMA((2, S)),
            DMA((2, S)),
            DMA((HH, S)),
            DMA((HH, S)),
            DMA((HH, 4)),
            DMA((HH, 4)),
            DMA((4,)),
            DMA((4,)),
            DMA((HH, half)),
            DMA((HH, half)),
            DMA((HH, half)),
            DMA((HH, half)),
            DMA((half,)),
            DMA((half,)),
            DMA((half,)),
            DMA((half,)),
            DMA((2, S)),
            DMA((2, S)),
            DMA((2, half, S)),
            DMA((2, half, S)),
        ],
        compiler_params=pltpu.CompilerParams(
            collective_id=0, has_side_effects=True, vmem_limit_bytes=63 * 1024 * 1024
        ),
    )(
        query[0],
        stretch_kv[:, 0],
        history_kv,
        block_mask,
        noise_level,
        history_blocks,
        out_weight.T,
        gate_table.T,
    )
    return out.T[None]


def solution(mesh):
    side = math.isqrt(mesh.shape["tp"])
    return jax.shard_map(
        functools.partial(on_device, side),
        mesh=mesh,
        in_specs=(
            P(("rep", "stretch"), "tp", None),
            P(None, ("rep", "stretch"), "tp", None),
            P(None, ("rep", "tp"), None),
            P(("rep", "stretch"), None, None),
            P(("rep", "stretch")),
            P("rep"),
            P(None, "tp"),
            P(None, "tp"),
        ),
        out_specs=P(("rep", "stretch"), None, "tp"),
        check_vma=False,
    )
```
